8 devices in a mesh: dp: 2 (over z, y), tp: 4 (over x, core).
Axes of the slice: x: 2, y: 2, z: 1, core: 2. Of those that a mesh axis runs over, the one named last changes fastest.
Arguments:
- x_in: bfloat16 [16384, 2048], P(('dp', 'tp')), parts along dimension 0
- w_in: bfloat16 [2048, 16384], P(None, 'tp')
- grad_out: bfloat16 [16384, 16384], P('dp', 'tp'), parts along dimension 0
Outputs:
- output 1: bfloat16 [16384, 2048], P(('dp', 'tp')), parts along dimension 0
- output 2: float32 [4096, 16384], P('dp', 'tp'), parts along dimension 0
There are 2 independent parts. The reference program is written for one: setup_inputs(seed, part) draws one part's arguments, and reference() takes and returns one part's arrays. A program takes and returns all parts, laid end to end along the dimension named above; an argument that names none is the same for every part.
All inputs are finite; a program needn't handle non-finite values.
Results may differ from the reference program's by a relative error of at most 0.001.
Values are sent between devices in bfloat16 or wider.
A program may use at most 1 GiB of HBM per device.

```python
import jax
import jax.numpy as jnp

TOKENS = 8192
HIDDEN = 2048
FFN_DIM = 16384


def setup_inputs(seed: int = 0, part: int = 0) -> dict:
    base_key = jax.random.key(seed)
    part_key = jax.random.fold_in(base_key, part)
    key_x, key_grad = jax.random.split(part_key)
    key_weight = jax.random.key(seed + 1)
    x_in = jax.random.normal(key_x, (TOKENS, HIDDEN), jnp.float32).astype(jnp.bfloat16)
    w_in = (jax.random.normal(key_weight, (HIDDEN, FFN_DIM), jnp.float32) * HIDDEN ** -0.5).astype(jnp.bfloat16)
    grad_scale = (HIDDEN / FFN_DIM) ** 0.5
    grad_out = (jax.random.normal(key_grad, (TOKENS, FFN_DIM), jnp.float32) * grad_scale).astype(jnp.bfloat16)
    return {"x_in": x_in, "w_in": w_in, "grad_out": grad_out}


def reference(x_in, w_in, grad_out):
    grad_x = jnp.dot(grad_out, w_in.T, preferred_element_type=jnp.float32).astype(jnp.bfloat16)
    grad_w = jnp.dot(x_in.T, grad_out, preferred_element_type=jnp.float32)
    return (grad_x, grad_w)
```

```python
import jax
import jax.numpy as jnp
from jax import lax
from jax.sharding import PartitionSpec as P


CHUNKS = (1536, 384, 96, 32)


def solution(mesh):
    tp_size = mesh.shape["tp"]
    sib_perm = [(t, t ^ 1) for t in range(tp_size)]
    peer_perm = [(t, t ^ 2) for t in range(tp_size)]

    def permute(value, perm):
        return lax.ppermute(value, "tp", perm)

    def half(value, core, rows):
        return lax.dynamic_slice_in_dim(value, core * rows, rows, 0, allow_negative_indices=False)

    def pair(mine, other, core):
        first = jnp.where(core == 0, mine, other)
        second = jnp.where(core == 0, other, mine)
        return jnp.concatenate((first, second), axis=0)

    def per_device(x_blk, w_blk, grad_blk):
        rows = x_blk.shape[0]
        me = lax.axis_index("tp")
        chip, core = me >> 1, me & 1

        def chip_rows(grad, which):
            return lax.dynamic_slice_in_dim(grad, which * 2 * rows, 2 * rows, 0, allow_negative_indices=False)

        def partial(grad, which):
            return lax.dot_general(
                chip_rows(grad, which), w_blk, (((1,), (1,)), ((), ())),
                preferred_element_type=jnp.float32)

        def weight_term(x_rows, grad, which):
            return lax.dot_general(
                x_rows, chip_rows(grad, which), (((0,), (0,)), ((), ())),
                preferred_element_type=jnp.float32)

        x_peer = permute(x_blk, peer_perm)
        x_sib = permute(x_blk, sib_perm)
        x_opp = permute(x_peer, sib_perm)

        remote = partial(grad_blk, chip ^ 1)
        from_sib = permute(half(remote, core ^ 1, rows), sib_perm)
        chip_sum = half(remote, core, rows) + from_sib
        arrived, start = [], 0
        for size in CHUNKS:
            arrived.append(permute(chip_sum[start:start + size], peer_perm))
            start += size

        grad_late, _ = lax.optimization_barrier((grad_blk, chip_sum))
        local = partial(grad_late, chip)
        own = half(local, core, rows) + permute(half(local, core ^ 1, rows), sib_perm)

        grad_w = weight_term(pair(x_blk, x_sib, core), grad_late, chip)
        grad_w = grad_w + weight_term(pair(x_peer, x_opp, core), grad_late, chip ^ 1)

        grad_x, start = jnp.zeros(x_blk.shape, jnp.bfloat16), 0
        for size, part in zip(CHUNKS, arrived):
            done = (own[start:start + size] + part).astype(jnp.bfloat16)
            grad_x = lax.dynamic_update_slice_in_dim(grad_x, done, start, 0)
            start += size
        return grad_x, grad_w

    return jax.shard_map(
        per_device,
        mesh=mesh,
        in_specs=(P(("dp", "tp"), None), P(None, "tp"), P("dp", "tp")),
        out_specs=(P(("dp", "tp"), None), P("dp", "tp")),
        check_vma=False,
    )
```

```python
import jax
import jax.numpy as jnp
from jax import lax
from jax.sharding import PartitionSpec as P


CHUNKS = (1536, 384, 96, 32)


def solution(mesh):
    tp_size = mesh.shape["tp"]
    sib_perm = [(t, t ^ 1) for t in range(tp_size)]
    peer_perm = [(t, t ^ 2) for t in range(tp_size)]

    def permute(value, perm):
        return lax.ppermute(value, "tp", perm)

    def half(value, core, rows):
        return lax.dynamic_slice_in_dim(value, core * rows, rows, 0, allow_negative_indices=False)

    def pair(mine, other, core):
        first = jnp.where(core == 0, mine, other)
        second = jnp.where(core == 0, other, mine)
        return jnp.concatenate((first, second), axis=0)

    def per_device(x_blk, w_blk, grad_blk):
        rows = x_blk.shape[0]
        me = lax.axis_index("tp")
        chip, core = me >> 1, me & 1

        def chip_rows(grad, which):
            return lax.dynamic_slice_in_dim(grad, which * 2 * rows, 2 * rows, 0, allow_negative_indices=False)

        def partial(grad, which):
            return lax.dot_general(
                chip_rows(grad, which), w_blk, (((1,), (1,)), ((), ())),
                preferred_element_type=jnp.float32)

        def weight_term(x_rows, grad, which):
            return lax.dot_general(
                x_rows, chip_rows(grad, which), (((0,), (0,)), ((), ())),
                preferred_element_type=jnp.float32)

        x_peer = permute(x_blk, peer_perm)
        x_sib = permute(x_blk, sib_perm)
        x_opp = permute(x_peer, sib_perm)

        remote = partial(grad_blk, chip ^ 1)
        from_sib = permute(half(remote, core ^ 1, rows), sib_perm)
        sums, arrived, start = [], [], 0
        for size in CHUNKS:
            mine = lax.dynamic_slice_in_dim(remote, core * rows + start, size, 0, allow_negative_indices=False)
            sums.append(mine + from_sib[start:start + size])
            arrived.append(permute(sums[-1], peer_perm))
            start += size

        grad_late, *_ = lax.optimization_barrier((grad_blk, *sums))
        local = partial(grad_late, chip)
        own = half(local, core, rows) + permute(half(local, core ^ 1, rows), sib_perm)

        x_local = pair(x_blk, x_sib, core)
        grad_w = weight_term(x_local, grad_late, chip)
        grad_w = grad_w + weight_term(pair(x_peer, x_opp, core), grad_late, chip ^ 1)

        grad_x, start = jnp.zeros(x_blk.shape, jnp.bfloat16), 0
        for size, part in zip(CHUNKS, arrived):
            done = (own[start:start + size] + part).astype(jnp.bfloat16)
            grad_x = lax.dynamic_update_slice_in_dim(grad_x, done, start, 0)
            start += size
        return grad_x, grad_w

    return jax.shard_map(
        per_device,
        mesh=mesh,
        in_specs=(P(("dp", "tp"), None), P(None, "tp"), P("dp", "tp")),
        out_specs=(P(("dp", "tp"), None), P("dp", "tp")),
        check_vma=False,
    )
```

```python
import jax
import jax.numpy as jnp
from jax import lax
from jax.sharding import PartitionSpec as P


CHUNKS = (1536, 384, 80, 32)
EXTRA = 16


def solution(mesh):
    tp_size = mesh.shape["tp"]
    sib_perm = [(t, t ^ 1) for t in range(tp_size)]
    peer_perm = [(t, t ^ 2) for t in range(tp_size)]
    core1 = [t for t in range(tp_size) if t % 2 == 1]

    def permute(value, perm):
        return lax.ppermute(value, "tp", perm)

    def half(value, core, rows):
        return lax.dynamic_slice_in_dim(value, core * rows, rows, 0, allow_negative_indices=False)

    def pair(mine, other, core):
        first = jnp.where(core == 0, mine, other)
        second = jnp.where(core == 0, other, mine)
        return jnp.concatenate((first, second), axis=0)

    def per_device(x_blk, w_blk, grad_blk):
        rows = x_blk.shape[0]
        me = lax.axis_index("tp")
        chip, core = me >> 1, me & 1

        def chip_rows(grad, which):
            return lax.dynamic_slice_in_dim(grad, which * 2 * rows, 2 * rows, 0, allow_negative_indices=False)

        def partial(grad, which):
            return lax.dot_general(
                chip_rows(grad, which), w_blk, (((1,), (1,)), ((), ())),
                preferred_element_type=jnp.float32)

        def weight_term(x_rows, grad, which):
            return lax.dot_general(
                x_rows, chip_rows(grad, which), (((0,), (0,)), ((), ())),
                preferred_element_type=jnp.float32)

        x_peer = permute(x_blk, peer_perm)
        x_sib = permute(x_blk, sib_perm)
        x_opp = permute(x_peer, sib_perm)

        remote = partial(grad_blk, chip ^ 1)
        from_sib = permute(half(remote, core ^ 1, rows), sib_perm)
        sums, arrived, start = [], [], 0
        for size in CHUNKS:
            mine = lax.dynamic_slice_in_dim(remote, core * rows + start, size, 0, allow_negative_indices=False)
            sums.append(mine + from_sib[start:start + size])
            arrived.append(permute(sums[-1], peer_perm))
            start += size

        last = remote[rows - EXTRA:rows]
        last = last + permute(last, [(t ^ 1, t) for t in core1])
        mine = remote[2 * rows - EXTRA:] + from_sib[rows - EXTRA:]
        last = permute(jnp.concatenate((last, mine)), [(t, t ^ 2) for t in core1])

        grad_late, *_ = lax.optimization_barrier((grad_blk, *sums))
        local = partial(grad_late, chip)
        own = half(local, core, rows) + permute(half(local, core ^ 1, rows), sib_perm)

        x_local = pair(x_blk, x_sib, core)
        grad_w = weight_term(x_local, grad_late, chip)
        grad_w = grad_w + weight_term(pair(x_peer, x_opp, core), grad_late, chip ^ 1)

        to_core0 = permute(last[:EXTRA], [(t, t ^ 1) for t in core1])
        arrived.insert(0, jnp.where(core == 0, to_core0, last[EXTRA:]))
        grad_x, start = jnp.zeros(x_blk.shape, jnp.bfloat16), rows - EXTRA
        for size, part in zip((EXTRA,) + CHUNKS, arrived):
            done = (own[start:start + size] + part).astype(jnp.bfloat16)
            grad_x = lax.dynamic_update_slice_in_dim(grad_x, done, start, 0)
            start = (start + size) % rows
        return grad_x, grad_w

    return jax.shard_map(
        per_device,
        mesh=mesh,
        in_specs=(P(("dp", "tp"), None), P(None, "tp"), P("dp", "tp")),
        out_specs=(P(("dp", "tp"), None), P("dp", "tp")),
        check_vma=False,
    )
```

```python
import jax
import jax.numpy as jnp
from jax import lax
from jax.experimental import pallas as pl
from jax.experimental.pallas import tpu as pltpu
from jax.sharding import PartitionSpec as P


CHUNKS = (1600, 368, 64)
EXTRA = 16


def add_rows(start, part, own, grad_x):
    size = part.shape[0]

    def kernel(part_ref, own_ref, _, out_ref, total, sem):
        total[...] = (own_ref[...] + part_ref[...]).astype(total.dtype)
        copy = pltpu.make_async_copy(total, out_ref.at[pl.ds(start, size)], sem)
        copy.start()
        copy.wait()

    return pl.pallas_call(
        kernel,
        out_shape=jax.ShapeDtypeStruct(grad_x.shape, grad_x.dtype),
        in_specs=[pl.BlockSpec(memory_space=pltpu.VMEM)] * 2 + [pl.BlockSpec(memory_space=pl.ANY)],
        out_specs=pl.BlockSpec(memory_space=pl.ANY),
        scratch_shapes=[pltpu.VMEM(part.shape, grad_x.dtype), pltpu.SemaphoreType.DMA],
        input_output_aliases={2: 0},
        cost_estimate=pl.CostEstimate(flops=part.size, bytes_accessed=10 * part.size, transcendentals=0),
        name="add_rows",
    )(pltpu.with_memory_space_constraint(part, pltpu.VMEM), pltpu.with_memory_space_constraint(own, pltpu.VMEM), grad_x)


def solution(mesh):
    tp_size = mesh.shape["tp"]
    sib_perm = [(t, t ^ 1) for t in range(tp_size)]
    peer_perm = [(t, t ^ 2) for t in range(tp_size)]
    core1 = [t for t in range(tp_size) if t % 2 == 1]

    def permute(value, perm):
        return lax.ppermute(value, "tp", perm)

    def half(value, core, rows):
        return lax.dynamic_slice_in_dim(value, core * rows, rows, 0, allow_negative_indices=False)

    def pair(mine, other, core):
        first = jnp.where(core == 0, mine, other)
        second = jnp.where(core == 0, other, mine)
        return jnp.concatenate((first, second), axis=0)

    def per_device(x_blk, w_blk, grad_blk):
        rows = x_blk.shape[0]
        me = lax.axis_index("tp")
        chip, core = me >> 1, me & 1

        def chip_rows(grad, which):
            return lax.dynamic_slice_in_dim(grad, which * 2 * rows, 2 * rows, 0, allow_negative_indices=False)

        def partial(grad, which):
            return lax.dot_general(
                chip_rows(grad, which), w_blk, (((1,), (1,)), ((), ())),
                preferred_element_type=jnp.float32)

        def weight_term(x_rows, grad, which):
            return lax.dot_general(
                x_rows, chip_rows(grad, which), (((0,), (0,)), ((), ())),
                preferred_element_type=jnp.float32)

        x_peer = permute(x_blk, peer_perm)
        x_sib = permute(x_blk, sib_perm)
        x_opp = permute(x_peer, sib_perm)

        remote = partial(grad_blk, chip ^ 1)
        from_sib = permute(half(remote, core ^ 1, rows), sib_perm)
        sums, arrived, start = [], [], 0
        for i, size in enumerate(CHUNKS):
            mine = lax.dynamic_slice_in_dim(remote, core * rows + start, size, 0, allow_negative_indices=False)
            sums.append(mine + from_sib[start:start + size])
            if i < len(CHUNKS) - 1:
                arrived.append(permute(sums[-1], peer_perm))
            start += size

        last = remote[rows - EXTRA:rows]
        last = last + permute(last, [(t ^ 1, t) for t in core1])
        mine = remote[2 * rows - EXTRA:] + from_sib[rows - EXTRA:]
        last = permute(jnp.concatenate((last, mine)), [(t, t ^ 2) for t in core1])

        grad_late, *_ = lax.optimization_barrier((grad_blk, *sums[:-1]))
        local = partial(grad_late, chip)
        own = half(local, core, rows) + permute(half(local, core ^ 1, rows), sib_perm)

        x_local = pair(x_blk, x_sib, core)
        grad_w = weight_term(x_local, grad_late, chip)
        grad_w = grad_w + weight_term(pair(x_peer, x_opp, core), grad_late, chip ^ 1)

        final, grad_w = lax.optimization_barrier((sums[-1], grad_w))
        arrived.append(permute(final, peer_perm))
        to_core0 = permute(last[:EXTRA], [(t, t ^ 1) for t in core1])
        arrived.insert(0, jnp.where(core == 0, to_core0, last[EXTRA:]))
        grad_x, start = jnp.zeros(x_blk.shape, jnp.bfloat16), rows - EXTRA
        for size, part in zip((EXTRA,) + CHUNKS, arrived):
            if part is arrived[-1]:
                grad_x = add_rows(start, part, own[start:start + size], grad_x)
                break
            done = (own[start:start + size] + part).astype(jnp.bfloat16)
            grad_x = lax.dynamic_update_slice_in_dim(grad_x, done, start, 0)
            start = (start + size) % rows
        return grad_x, grad_w

    return jax.shard_map(
        per_device,
        mesh=mesh,
        in_specs=(P(("dp", "tp"), None), P(None, "tp"), P("dp", "tp")),
        out_specs=(P(("dp", "tp"), None), P("dp", "tp")),
        check_vma=False,
    )
```

```python
import jax
import jax.numpy as jnp
from jax import lax
from jax.experimental import pallas as pl
from jax.experimental.pallas import tpu as pltpu
from jax.sharding import PartitionSpec as P


CHUNKS = (1552, 432, 48)
EXTRA = 16
PIECE = 16


def add_rows(start, part, own, grad_x):
    size = part.shape[0]

    def kernel(part_ref, own_ref, _, out_ref, total, sems):
        copies = []
        for i in range(size // PIECE):
            rows = pl.ds(i * PIECE, PIECE)
            total[rows] = (own_ref[rows] + part_ref[rows]).astype(total.dtype)
            copies.append(pltpu.make_async_copy(
                total.at[rows], out_ref.at[pl.ds(start + i * PIECE, PIECE)], sems.at[i]))
            copies[-1].start()
        for copy in copies:
            copy.wait()

    return pl.pallas_call(
        kernel,
        out_shape=jax.ShapeDtypeStruct(grad_x.shape, grad_x.dtype),
        in_specs=[pl.BlockSpec(memory_space=pltpu.VMEM)] * 2 + [pl.BlockSpec(memory_space=pl.ANY)],
        out_specs=pl.BlockSpec(memory_space=pl.ANY),
        scratch_shapes=[pltpu.VMEM(part.shape, grad_x.dtype), pltpu.SemaphoreType.DMA((size // PIECE,))],
        input_output_aliases={2: 0},
        cost_estimate=pl.CostEstimate(flops=part.size, bytes_accessed=10 * part.size, transcendentals=0),
        name="add_rows",
    )(pltpu.with_memory_space_constraint(part, pltpu.VMEM), pltpu.with_memory_space_constraint(own, pltpu.VMEM), grad_x)


def solution(mesh):
    tp_size = mesh.shape["tp"]
    sib_perm = [(t, t ^ 1) for t in range(tp_size)]
    peer_perm = [(t, t ^ 2) for t in range(tp_size)]
    core1 = [t for t in range(tp_size) if t % 2 == 1]

    def permute(value, perm):
        return lax.ppermute(value, "tp", perm)

    def half(value, core, rows):
        return lax.dynamic_slice_in_dim(value, core * rows, rows, 0, allow_negative_indices=False)

    def pair(mine, other, core):
        first = jnp.where(core == 0, mine, other)
        second = jnp.where(core == 0, other, mine)
        return jnp.concatenate((first, second), axis=0)

    def per_device(x_blk, w_blk, grad_blk):
        rows = x_blk.shape[0]
        me = lax.axis_index("tp")
        chip, core = me >> 1, me & 1

        def chip_rows(grad, which):
            return lax.dynamic_slice_in_dim(grad, which * 2 * rows, 2 * rows, 0, allow_negative_indices=False)

        def partial(grad, which):
            return lax.dot_general(
                chip_rows(grad, which), w_blk, (((1,), (1,)), ((), ())),
                preferred_element_type=jnp.float32)

        def weight_term(x_rows, grad, which):
            return lax.dot_general(
                x_rows, chip_rows(grad, which), (((0,), (0,)), ((), ())),
                preferred_element_type=jnp.float32)

        x_peer = permute(x_blk, peer_perm)
        x_sib = permute(x_blk, sib_perm)
        x_opp = permute(x_peer, sib_perm)

        remote = partial(grad_blk, chip ^ 1)
        from_sib = permute(half(remote, core ^ 1, rows), sib_perm)
        sums, arrived, start = [], [], 0
        for i, size in enumerate(CHUNKS):
            mine = lax.dynamic_slice_in_dim(remote, core * rows + start, size, 0, allow_negative_indices=False)
            sums.append(mine + from_sib[start:start + size])
            if i < len(CHUNKS) - 1:
                arrived.append(permute(sums[-1], peer_perm))
            start += size

        last = remote[rows - EXTRA:rows]
        last = last + permute(last, [(t ^ 1, t) for t in core1])
        mine = remote[2 * rows - EXTRA:] + from_sib[rows - EXTRA:]
        last = permute(jnp.concatenate((last, mine)), [(t, t ^ 2) for t in core1])

        grad_late, *_ = lax.optimization_barrier((grad_blk, *sums[:-1]))
        local = partial(grad_late, chip)
        own = half(local, core, rows) + permute(half(local, core ^ 1, rows), sib_perm)

        x_local = pair(x_blk, x_sib, core)
        grad_w = weight_term(x_local, grad_late, chip)
        grad_w = grad_w + weight_term(pair(x_peer, x_opp, core), grad_late, chip ^ 1)

        final, grad_w = lax.optimization_barrier((sums[-1], grad_w))
        arrived.append(permute(final, peer_perm))
        to_core0 = permute(last, [(t, t ^ 1) for t in core1])
        arrived.insert(0, jnp.where(core == 0, to_core0[:EXTRA], last[EXTRA:]))
        grad_x, start = jnp.zeros(x_blk.shape, jnp.bfloat16), rows - EXTRA
        for size, part in zip((EXTRA,) + CHUNKS, arrived):
            if part is arrived[-1]:
                grad_x = add_rows(start, part, own[start:start + size], grad_x)
                break
            done = (own[start:start + size] + part).astype(jnp.bfloat16)
            grad_x = lax.dynamic_update_slice_in_dim(grad_x, done, start, 0)
            start = (start + size) % rows
        return grad_x, grad_w

    return jax.shard_map(
        per_device,
        mesh=mesh,
        in_specs=(P(("dp", "tp"), None), P(None, "tp"), P("dp", "tp")),
        out_specs=(P(("dp", "tp"), None), P("dp", "tp")),
        check_vma=False,
    )
```
